32 devices in a mesh: px: 8 (over y, x, core), py: 4 (over z).
Axes of the slice: x: 2, y: 2, z: 4, core: 2. Of those that a mesh axis runs over, the one named last changes fastest.
Arguments:
- source: float32 [1024, 512, 128], P('px', 'py'), may hold values from -8 to 8
- layer_mass: float32 [128], replicated, may hold values from 0.5 to 4
- modes: float32 [128, 128], replicated, may hold values from -0.5 to 0.5
- mode_eigen: float32 [128], replicated, may hold values from 0.0002 to 1
Outputs:
- solution: float32 [1024, 512, 128], P('px', 'py')
The draws below stay inside these ranges and needn't reach their ends.
All inputs are finite; a program needn't handle non-finite values.
Results may differ from the reference program's by a relative error of at most 0.0014.
Values sent between devices are 32-bit elements; how exact they have to be, the bound alone decides.
A program may use at most 128 MiB of HBM per device.

```python
import math
import jax
import jax.numpy as jnp
from jax import lax

NX = 1024
NY = 512
NZ = 128


def draw_source(key, part):
    first = jax.random.fold_in(key, 0)
    values = jax.random.normal(first, (NX, NY, NZ), jnp.float32)
    return jnp.clip(values, -8.0, 8.0).astype(jnp.float32)


def normal_values(stream_key, dims, scale, reach, kind=jnp.bfloat16):
    entries = scale * jax.random.normal(stream_key, dims, jnp.float32)
    return jnp.clip(entries, min=-reach, max=reach).astype(kind)


def setup_inputs(seed: int = 0) -> dict:
    arg_keys = jax.random.split(jax.random.key(seed), 5)
    return {
        "source": draw_source(jax.random.fold_in(arg_keys[4], 71), 0),
        "layer_mass": jnp.clip(jnp.exp(jax.random.uniform(arg_keys[1], (NZ,), jnp.float32, math.log(0.5), math.log(4.0))), 0.5, 4.0),
        "modes": normal_values(arg_keys[2], (NZ, NZ), NZ ** -0.5, 0.5, jnp.float32),
        "mode_eigen": jnp.clip(jnp.exp(jax.random.uniform(arg_keys[3], (NZ,), jnp.float32, math.log(0.0002), math.log(1.0))), 0.0002, 1.0),
    }


def cosine_table(length):
    rows = jnp.arange(length, dtype=jnp.float32)[:, None]
    cols = jnp.arange(length, dtype=jnp.float32)[None, :]
    scale = jnp.where(rows == 0.0, jnp.sqrt(1.0 / length), jnp.sqrt(2.0 / length)).astype(jnp.float32)
    return (scale * jnp.cos(jnp.pi * (cols + 0.5) * rows / length)).astype(jnp.float32)

def laplace_eigen(length):
    waves = jnp.arange(length, dtype=jnp.float32)
    return (2.0 - 2.0 * jnp.cos(jnp.pi * waves / length)).astype(jnp.float32)

def reference(source, layer_mass, modes, mode_eigen):
    high = lax.Precision.HIGHEST
    table_x = cosine_table(NX)
    table_y = cosine_table(NY)
    wave_x = laplace_eigen(NX)
    wave_y = laplace_eigen(NY)
    weighted = source * layer_mass
    modal_field = jnp.einsum('xyz,zk->kxy', weighted, modes, precision=high)

    def solve_mode(packed):
        planes, eigen_value = packed
        spectral = jnp.dot(jnp.dot(table_x, planes, precision=high), table_y.T, precision=high)
        scaled = spectral / (eigen_value + wave_x[:, None] + wave_y[None, :])
        return jnp.dot(jnp.dot(table_x.T, scaled, precision=high), table_y, precision=high)
    returned = lax.map(solve_mode, (modal_field, mode_eigen))
    return jnp.einsum('kxy,zk->xyz', returned, modes, precision=high)
```

```python
import jax
import jax.numpy as jnp
import numpy as np
from jax import lax
from jax.sharding import PartitionSpec as P

HIGH = lax.Precision.HIGH


def cosine_table(length):
    rows = np.arange(length, dtype=np.float64)[:, None]
    cols = np.arange(length, dtype=np.float64)[None, :]
    scale = np.where(rows == 0.0, np.sqrt(1.0 / length), np.sqrt(2.0 / length))
    return scale * np.cos(np.pi * (cols + 0.5) * rows / length)


def laplace_eigen(length):
    return 4.0 * np.sin(0.5 * np.pi * np.arange(length, dtype=np.float64) / length) ** 2


def sine_table(count):
    m = np.arange(1, count + 1, dtype=np.float64)
    table = np.sqrt(2.0 / (count + 1)) * np.sin(np.pi * np.outer(m, m) / (count + 1))
    return table, np.cos(np.pi * m / (count + 1))


def f32(table):
    return jnp.asarray(np.asarray(table, dtype=np.float32))


def mul(spec, *arrays):
    return jnp.einsum(spec, *arrays, precision=HIGH, preferred_element_type=jnp.float32)


def edges(table):
    return np.stack([table[:, 0], table[:, -1]])


def interfaces(xe, ye, eigen, bx, by):
    count_x, count_y = xe.shape[:2]
    cx, cy = cosine_table(bx), cosine_table(by)
    ex, ey = edges(cx), edges(cy)
    mu, nu = laplace_eigen(bx), laplace_eigen(by)
    nu_all = laplace_eigen(by * count_y)
    whole = cosine_table(by * count_y).reshape(by * count_y, count_y, by)
    turn = f32(np.einsum("bjy,qy->bjq", whole, cy))
    inverse = 1.0 / (eigen[:, None, None] + f32(mu[:, None] + nu[None, :]))
    inverse_all = 1.0 / (eigen[:, None, None] + f32(mu[:, None] + nu_all[None, :]))
    ex32, ey32 = f32(ex), f32(ey)
    sin_x, cos_x = (f32(t) for t in sine_table(count_x - 1))
    sin_y, cos_y = (f32(t) for t in sine_table(count_y - 1))

    own_y = jnp.sum(inverse * f32(ey[0] * ey[0]), -1)
    far_y = jnp.sum(inverse * f32(ey[0] * ey[1]), -1)
    gain_y = 1.0 / (1.0 + 2.0 * own_y[:, None] - 2.0 * far_y[:, None] * cos_y[None, :, None])
    own_x = jnp.sum(inverse_all * f32(ex[0] * ex[0])[:, None], 1)
    far_x = jnp.sum(inverse_all * f32(ex[0] * ex[1])[:, None], 1)
    gain_x = 1.0 / (1.0 + 2.0 * own_x[:, None] - 2.0 * far_x[:, None] * cos_x[None, :, None])

    def solve_y(values):
        jump = values[:, 1:, :, 0] - values[:, :-1, :, 1]
        modal = mul("ml,ilnp->imnp", sin_y, jump) * gain_y.transpose(1, 0, 2)
        return mul("ml,ilnp->imnp", sin_y, modal)

    def loads_y(w):
        first = jnp.pad(w, ((0, 0), (1, 0), (0, 0), (0, 0)))
        last = jnp.pad(w, ((0, 0), (0, 1), (0, 0), (0, 0)))
        return jnp.stack([first, -last], 3)

    def loads_x(w):
        first = jnp.pad(w, ((1, 0), (0, 0), (0, 0), (0, 0)))
        last = jnp.pad(w, ((0, 1), (0, 0), (0, 0), (0, 0)))
        return jnp.stack([first, -last], 3)

    wy = solve_y(ye)
    load = loads_y(wy)
    weighted = load[:, :, :, None] * ex32[:, None, :]
    moved = mul("ijnfep,npq->ijnfeq", weighted, inverse)
    xs = xe - jnp.sum(moved * ey32, 4)
    jump = xs[1:, :, :, 0] - xs[:-1, :, :, 1]
    spectral = mul("ijnq,bjq->inb", jump, turn)
    spectral = mul("ml,lnb->mnb", sin_x, spectral) * gain_x.transpose(1, 0, 2)
    spectral = mul("ml,lnb->mnb", sin_x, spectral)
    wx = mul("inb,bjq->ijnq", spectral, turn)
    xload = loads_x(wx)
    weighted = xload[:, :, :, None] * ey32[:, None, :]
    moved = mul("ijnfeq,npq->ijnfep", weighted, inverse)
    wy = wy - solve_y(jnp.sum(moved * ex32, 4))
    return xload, loads_y(wy)


def shards(source, layer_mass, modes, mode_eigen):
    bx, by, levels = source.shape
    count_x = lax.axis_size("px")
    count_y = lax.axis_size("py")
    devices = count_x * count_y
    group = levels // devices
    cx, cy = cosine_table(bx), cosine_table(by)
    mu, nu = laplace_eigen(bx), laplace_eigen(by)
    cx32, cy32, ex, ey = f32(cx), f32(cy), f32(edges(cx)), f32(edges(cy))

    field = mul("xyz,zk->xyk", source, layer_mass[:, None] * modes)
    field = mul("qy,xyk->xqk", cy32, field)
    field = mul("px,xqk->pqk", cx32, field)
    inverse = 1.0 / (mode_eigen + f32(mu[:, None] + nu[None, :])[:, :, None])
    local = field * inverse
    xe = jnp.stack([jnp.sum(local * e[:, None, None], 0) for e in ex])
    ye = jnp.stack([jnp.sum(local * e[:, None], 1) for e in ey])

    packed = jnp.concatenate([xe.reshape(2 * by, levels), ye.reshape(2 * bx, levels)]).T
    sent = packed.reshape(devices, group, 2 * (bx + by))
    got = lax.all_to_all(sent, ("px", "py"), split_axis=0, concat_axis=0, tiled=True)
    got = got.reshape(count_x, count_y, group, 2 * (bx + by))
    first_mode = (lax.axis_index("px") * count_y + lax.axis_index("py")) * group
    eigen = lax.dynamic_slice_in_dim(mode_eigen, first_mode, group)
    xl, yl = interfaces(
        got[..., : 2 * by].reshape(count_x, count_y, group, 2, by),
        got[..., 2 * by :].reshape(count_x, count_y, group, 2, bx),
        eigen,
        bx,
        by,
    )
    back = jnp.concatenate(
        [xl.reshape(devices, group, 2 * by), yl.reshape(devices, group, 2 * bx)], 2
    )
    back = lax.all_to_all(back, ("px", "py"), split_axis=0, concat_axis=0, tiled=True)
    back = back.reshape(levels, 2 * (bx + by)).T
    xl = back[: 2 * by].reshape(2, by, levels)
    yl = back[2 * by :].reshape(2, bx, levels)

    load = ex[0][:, None, None] * xl[0] + ex[1][:, None, None] * xl[1]
    load = load + ey[0][:, None] * yl[0][:, None] + ey[1][:, None] * yl[1][:, None]
    local = local - load * inverse
    local = mul("px,pqk->xqk", cx32, local)
    local = mul("qy,xqk->xyk", cy32, local)
    return mul("xyk,zk->xyz", local, modes)


def solution(mesh):
    placed = (P("px", "py", None), P(), P(), P())
    return jax.shard_map(
        shards, mesh=mesh, in_specs=placed, out_specs=P("px", "py", None), check_vma=False
    )
```

```python
import functools

import jax
import jax.numpy as jnp
import numpy as np
from jax import lax
from jax.experimental import pallas as pl
from jax.experimental.pallas import tpu as pltpu
from jax.sharding import PartitionSpec as P

HIGH = lax.Precision.HIGH


def cosine_table(length):
    rows = np.arange(length, dtype=np.float64)[:, None]
    cols = np.arange(length, dtype=np.float64)[None, :]
    scale = np.where(rows == 0.0, np.sqrt(1.0 / length), np.sqrt(2.0 / length))
    return scale * np.cos(np.pi * (cols + 0.5) * rows / length)


def laplace_eigen(length):
    return 4.0 * np.sin(0.5 * np.pi * np.arange(length, dtype=np.float64) / length) ** 2


def sine_table(count):
    m = np.arange(1, count + 1, dtype=np.float64)
    table = np.sqrt(2.0 / (count + 1)) * np.sin(np.pi * np.outer(m, m) / (count + 1))
    return table, np.cos(np.pi * m / (count + 1))


def f32(table):
    return jnp.asarray(np.asarray(table, dtype=np.float32))


def mul(spec, *arrays):
    return jnp.einsum(spec, *arrays, precision=HIGH, preferred_element_type=jnp.float32)


def edges(table):
    return np.stack([table[:, 0], table[:, -1]])


def interfaces(xe, ye, eigen, bx, by):
    count_x, count_y = xe.shape[:2]
    cx, cy = cosine_table(bx), cosine_table(by)
    ex, ey = edges(cx), edges(cy)
    mu, nu = laplace_eigen(bx), laplace_eigen(by)
    nu_all = laplace_eigen(by * count_y)
    whole = cosine_table(by * count_y).reshape(by * count_y, count_y, by)
    turn = f32(np.einsum("bjy,qy->bjq", whole, cy))
    inverse = 1.0 / (eigen[:, None, None] + f32(mu[:, None] + nu[None, :]))
    inverse_all = 1.0 / (eigen[:, None, None] + f32(mu[:, None] + nu_all[None, :]))
    ex32, ey32 = f32(ex), f32(ey)
    sin_x, cos_x = (f32(t) for t in sine_table(count_x - 1))
    sin_y, cos_y = (f32(t) for t in sine_table(count_y - 1))

    own_y = jnp.sum(inverse * f32(ey[0] * ey[0]), -1)
    far_y = jnp.sum(inverse * f32(ey[0] * ey[1]), -1)
    gain_y = 1.0 / (1.0 + 2.0 * own_y[:, None] - 2.0 * far_y[:, None] * cos_y[None, :, None])
    own_x = jnp.sum(inverse_all * f32(ex[0] * ex[0])[:, None], 1)
    far_x = jnp.sum(inverse_all * f32(ex[0] * ex[1])[:, None], 1)
    gain_x = 1.0 / (1.0 + 2.0 * own_x[:, None] - 2.0 * far_x[:, None] * cos_x[None, :, None])

    def solve_y(values):
        jump = values[:, 1:, :, 0] - values[:, :-1, :, 1]
        modal = mul("ml,ilnp->imnp", sin_y, jump) * gain_y.transpose(1, 0, 2)
        return mul("ml,ilnp->imnp", sin_y, modal)

    def loads_y(w):
        first = jnp.pad(w, ((0, 0), (1, 0), (0, 0), (0, 0)))
        last = jnp.pad(w, ((0, 0), (0, 1), (0, 0), (0, 0)))
        return jnp.stack([first, -last], 3)

    def loads_x(w):
        first = jnp.pad(w, ((1, 0), (0, 0), (0, 0), (0, 0)))
        last = jnp.pad(w, ((0, 1), (0, 0), (0, 0), (0, 0)))
        return jnp.stack([first, -last], 3)

    wy = solve_y(ye)
    load = loads_y(wy)
    weighted = load[:, :, :, None] * ex32[:, None, :]
    moved = mul("ijnfep,npq->ijnfeq", weighted, inverse)
    xs = xe - jnp.sum(moved * ey32, 4)
    jump = xs[1:, :, :, 0] - xs[:-1, :, :, 1]
    spectral = mul("ijnq,bjq->inb", jump, turn)
    spectral = mul("ml,lnb->mnb", sin_x, spectral) * gain_x.transpose(1, 0, 2)
    spectral = mul("ml,lnb->mnb", sin_x, spectral)
    wx = mul("inb,bjq->ijnq", spectral, turn)
    xload = loads_x(wx)
    weighted = xload[:, :, :, None] * ey32[:, None, :]
    moved = mul("ijnfeq,npq->ijnfep", weighted, inverse)
    wy = wy - solve_y(jnp.sum(moved * ex32, 4))
    return xload, loads_y(wy)


BF16 = jnp.bfloat16
F32 = jnp.float32


def split(values):
    high = values.astype(BF16)
    return high, (values - high.astype(F32)).astype(BF16)


def left_table(table):
    table = np.asarray(table, dtype=np.float32)
    high = table.astype(BF16)
    low = (table - high.astype(np.float32)).astype(BF16)
    return jnp.asarray(np.concatenate([high, high, low], 1))


def stack_rows(values):
    high, low = split(values)
    return jnp.concatenate([high, low, high], 0)


def times_right(values, factor):
    high, low = split(values)
    fhigh, flow = split(factor)
    return jnp.dot(
        jnp.concatenate([high, low, high], 1),
        jnp.concatenate([fhigh, fhigh, flow], 0),
        preferred_element_type=F32,
    )


def times_left(table, values):
    return jnp.dot(table, stack_rows(values), preferred_element_type=F32)


def forward_kernel(
    steps_x, xb, qb, nu_ref, ey_ref, source_ref, mass_ref, modes_ref, cx_ref, cy_ref, ex_ref,
    mu_ref, eigen_ref, local_ref, edges_ref, half_ref, even_ref, odd_ref, xe_ref,
):
    step = pl.program_id(0)
    by, levels = source_ref.shape[1:]
    bx = mu_ref.shape[0]

    @pl.when(step < steps_x)
    def _():
        field = times_right(
            source_ref[...].reshape(xb * by, levels) * mass_ref[...], modes_ref[...]
        )
        for x in range(0, xb, 2):
            pair = jnp.concatenate(
                [field[x * by : (x + 1) * by], field[(x + 1) * by : (x + 2) * by]], 1
            )
            pair = times_left(cy_ref[...], pair)
            row = pl.multiple_of((step * xb + x) * by, 2 * by)
            half_ref[pl.ds(row, by)] = pair[:, :levels]
            half_ref[pl.ds(row + by, by)] = pair[:, levels:]

    @pl.when(step == steps_x)
    def _():
        even_ref[...] = jnp.zeros_like(even_ref)
        odd_ref[...] = jnp.zeros_like(odd_ref)

    @pl.when(step >= steps_x)
    def _():
        first = (step - steps_x) * qb
        columns = jnp.concatenate(
            [half_ref[pl.ds(first + q, bx, stride=by), :] for q in range(qb)], 1
        )
        spectral = times_left(cx_ref[...], columns)
        base = mu_ref[...] + eigen_ref[...]
        weight = ex_ref[...]
        sums = [None, None]
        sign = jnp.where(
            lax.broadcasted_iota(jnp.int32, (8, levels), 0) % 2 == 0, 1.0, -1.0
        ).astype(F32)
        rows = [[], []]
        for q in range(qb):
            value = spectral[:, q * levels : (q + 1) * levels] / (base + nu_ref[first + q])
            local_ref[q] = value
            folded = jnp.sum((value * weight).reshape(bx // 8, 8, levels), 0)
            rows[0].append(jnp.sum(folded, 0, keepdims=True))
            rows[1].append(jnp.sum(folded * sign, 0, keepdims=True))
            term = value * ey_ref[first + q]
            sums[q % 2] = term if sums[q % 2] is None else sums[q % 2] + term
        even_ref[...] += sums[0]
        odd_ref[...] += sums[1]
        here = pl.ds(pl.multiple_of(first, qb), qb)
        xe_ref[0, here] = jnp.concatenate(rows[0], 0)
        xe_ref[1, here] = jnp.concatenate(rows[1], 0)

    @pl.when(step == pl.num_programs(0) - 1)
    def _():
        even, odd = even_ref[...], odd_ref[...]
        edges_ref[:, : 2 * by] = xe_ref[...].reshape(2 * by, levels).T
        edges_ref[:, 2 * by :] = jnp.concatenate([even + odd, even - odd], 0).T


def backward_kernel(
    steps_q, xb, qb, nu_ref, ey_ref, local_ref, modes_ref, cx_ref, cy_ref, ex_ref, mu_ref,
    eigen_ref, loads_ref, out_ref, half_ref, xl_ref, yl_ref, turned_ref,
):
    step = pl.program_id(0)
    bx, levels = mu_ref.shape
    by = xl_ref.shape[1]

    @pl.when(step == 0)
    def _():
        xl_ref[...] = loads_ref[:, : 2 * by].T.reshape(2, by, levels)
        yl_ref[...] = loads_ref[:, 2 * by :].T.reshape(2, bx, levels)
        turned_ref[...] = modes_ref[...].T

    @pl.when(step < steps_q)
    def _():
        first = step * qb
        base = mu_ref[...] + eigen_ref[...]
        weight = ex_ref[...]
        flip = jnp.where(
            lax.broadcasted_iota(jnp.int32, (bx, levels), 0) % 2 == 0, weight, -weight
        )
        here = pl.ds(pl.multiple_of(first, qb), qb)
        left, right = xl_ref[0, here], xl_ref[1, here]
        both = [yl_ref[0] + yl_ref[1], yl_ref[0] - yl_ref[1]]
        columns = []
        for q in range(qb):
            load = weight * left[q : q + 1] + flip * right[q : q + 1]
            load = load + ey_ref[first + q] * both[q % 2]
            columns.append(local_ref[q] - load / (base + nu_ref[first + q]))
        field = times_left(cx_ref[...], jnp.concatenate(columns, 1))
        for q in range(qb):
            half_ref[pl.ds(first + q, bx, stride=by), :] = field[:, q * levels : (q + 1) * levels]

    @pl.when(step >= steps_q)
    def _():
        parts = []
        for x in range(0, xb, 2):
            row = pl.multiple_of(((step - steps_q) * xb + x) * by, 2 * by)
            pair = jnp.concatenate([half_ref[pl.ds(row, by)], half_ref[pl.ds(row + by, by)]], 1)
            pair = times_left(cy_ref[...], pair)
            parts += [pair[:, :levels], pair[:, levels:]]
        field = jnp.concatenate(parts, 0)
        out_ref[...] = times_right(field, turned_ref[...]).reshape(xb, by, levels)


def whole_block(array):
    return pl.BlockSpec(array.shape, lambda i: (0,) * array.ndim)


SCALARS = pl.BlockSpec(memory_space=pltpu.SMEM)
VMEM_LIMIT = 56 * 1024 * 1024


def forward(source, mass, modes, cx, cy, ex, mu, eigen, nu, ey):
    bx, by, levels = source.shape
    xb, qb = min(32, bx), min(16, by)
    steps_x, steps_q = bx // xb, by // qb
    return pl.pallas_call(
        functools.partial(forward_kernel, steps_x, xb, qb),
        name="forward",
        grid=(steps_x + steps_q,),
        in_specs=[
            SCALARS,
            SCALARS,
            pl.BlockSpec((xb, by, levels), lambda i: (jnp.minimum(i, steps_x - 1), 0, 0)),
        ]
        + [whole_block(a) for a in (mass, modes, cx, cy, ex, mu, eigen)],
        out_specs=[
            pl.BlockSpec((qb, bx, levels), lambda i: (jnp.maximum(i - steps_x, 0), 0, 0)),
            pl.BlockSpec((levels, 2 * (bx + by)), lambda i: (0, 0)),
        ],
        out_shape=[
            jax.ShapeDtypeStruct((by, bx, levels), F32),
            jax.ShapeDtypeStruct((levels, 2 * (bx + by)), F32),
        ],
        scratch_shapes=[
            pltpu.VMEM((bx * by, levels), F32),
            pltpu.VMEM((bx, levels), F32),
            pltpu.VMEM((bx, levels), F32),
            pltpu.VMEM((2, by, levels), F32),
        ],
        compiler_params=pltpu.CompilerParams(vmem_limit_bytes=VMEM_LIMIT),
    )(nu, ey, source, mass, modes, cx, cy, ex, mu, eigen)


def backward(local, modes, cx, cy, ex, mu, eigen, nu, ey, loads):
    by, bx, levels = local.shape
    xb, qb = min(32, bx), min(16, by)
    steps_x, steps_q = bx // xb, by // qb
    return pl.pallas_call(
        functools.partial(backward_kernel, steps_q, xb, qb),
        name="backward",
        grid=(steps_x + steps_q,),
        in_specs=[
            SCALARS,
            SCALARS,
            pl.BlockSpec((qb, bx, levels), lambda i: (jnp.minimum(i, steps_q - 1), 0, 0)),
        ]
        + [whole_block(a) for a in (modes, cx, cy, ex, mu, eigen, loads)],
        out_specs=pl.BlockSpec((xb, by, levels), lambda i: (jnp.maximum(i - steps_q, 0), 0, 0)),
        out_shape=jax.ShapeDtypeStruct((bx, by, levels), F32),
        scratch_shapes=[
            pltpu.VMEM((bx * by, levels), F32),
            pltpu.VMEM((2, by, levels), F32),
            pltpu.VMEM((2, bx, levels), F32),
            pltpu.VMEM((levels, levels), F32),
        ],
        compiler_params=pltpu.CompilerParams(vmem_limit_bytes=VMEM_LIMIT),
    )(nu, ey, local, modes, cx, cy, ex, mu, eigen, loads)


def shards(source, layer_mass, modes, mode_eigen):
    bx, by, levels = source.shape
    count_x = lax.axis_size("px")
    count_y = lax.axis_size("py")
    devices = count_x * count_y
    group = levels // devices
    cx, cy = cosine_table(bx), cosine_table(by)
    mu, nu = laplace_eigen(bx), laplace_eigen(by)
    nu32, ey32 = f32(nu), f32(cy[:, 0])
    ex = f32(np.repeat(cx[:, :1], levels, 1))
    mu32 = f32(np.repeat(mu[:, None], levels, 1))
    eigen_row = mode_eigen.reshape(1, levels)

    local, packed = forward(
        source, layer_mass.reshape(1, levels), modes, left_table(cx), left_table(cy), ex, mu32,
        eigen_row, nu32, ey32,
    )
    sent = packed.reshape(devices, group, 2 * (bx + by))
    got = lax.all_to_all(sent, ("px", "py"), split_axis=0, concat_axis=0, tiled=True)
    got = got.reshape(count_x, count_y, group, 2 * (bx + by))
    first_mode = (lax.axis_index("px") * count_y + lax.axis_index("py")) * group
    eigen = lax.dynamic_slice_in_dim(mode_eigen, first_mode, group)
    xl, yl = interfaces(
        got[..., : 2 * by].reshape(count_x, count_y, group, 2, by),
        got[..., 2 * by :].reshape(count_x, count_y, group, 2, bx),
        eigen,
        bx,
        by,
    )
    back = jnp.concatenate(
        [xl.reshape(devices, group, 2 * by), yl.reshape(devices, group, 2 * bx)], 2
    )
    back = lax.all_to_all(back, ("px", "py"), split_axis=0, concat_axis=0, tiled=True)
    return backward(
        local, modes, left_table(cx.T), left_table(cy.T), ex, mu32, eigen_row, nu32, ey32,
        back.reshape(levels, 2 * (bx + by)),
    )


def solution(mesh):
    placed = (P("px", "py", None), P(), P(), P())
    return jax.shard_map(
        shards, mesh=mesh, in_specs=placed, out_specs=P("px", "py", None), check_vma=False
    )
```
